512 devices in a mesh: dp: 32 (over x, y), tensor: 16 (over z, core).
Axes of the slice: x: 4, y: 8, z: 8, core: 2. Of those that a mesh axis runs over, the one named last changes fastest.
Arguments:
- acts: bfloat16 [32768, 256], P('dp'), may hold values from -6 to 6
- out_grad: bfloat16 [32768, 16384], P('dp', 'tensor'), may hold values from -6 to 6
- weight: float32 [256, 16384], P(None, 'tensor'), may hold values from -0.375 to 0.375
- error: float32 [32, 256, 16384], P('dp', None, 'tensor'), may hold values from -6 to 6
- start_q: float32 [16384, 64], P('tensor'), may hold values from -0.1875 to 0.1875
Outputs:
- new_weight: float32 [256, 16384], P(None, 'tensor')
- new_error: float32 [32, 256, 16384], P('dp', None, 'tensor')
- input_grad: float32 [32768, 256], P(('dp', 'tensor'))
The draws below stay inside these ranges and needn't reach their ends.
All inputs are finite; a program needn't handle non-finite values.
Results may differ from the reference program's by a relative error of at most 0.0003.
Values sent between devices are 32-bit elements; how exact they have to be, the bound alone decides.
A program may use at most 64 MiB of HBM per device.

```python
import math
import jax
import jax.numpy as jnp
from jax import lax

DIN = 256
COL_DEV = 1024
RANK = 64
TOK_DEV = 1024
COLS = 16384
TOKENS = 32768
REPLICAS = 32
N_TENSOR = 16


def block_scale(key, dims, shards, least, top_value):
    def one(axis_at, parts):
        heights = jax.random.uniform(jax.random.fold_in(jax.random.fold_in(key, 6), axis_at), (parts,), jnp.float32, least / len(shards), top_value / len(shards))
        return jnp.repeat(jnp.exp(heights), dims[axis_at] // parts).reshape((-1,) + (1,) * (len(dims) - axis_at - 1))

    loudness = one(*shards[0])
    for cut in shards[1:]:
        loudness = loudness * one(*cut)
    return loudness


def gaussian(own_key, dims, width, bound, cuts=(), kind=jnp.bfloat16):
    drawn = width * jax.random.normal(own_key, dims, jnp.float32)
    if cuts:
        drawn = drawn * block_scale(own_key, dims, cuts, -0.22, 0.18)
    return jnp.clip(drawn, -bound, bound).astype(kind)


def setup_inputs(seed: int = 0) -> dict:
    key_list = jax.random.split(jax.random.key(seed), 6)
    acts = gaussian(key_list[0], (TOKENS, DIN), 1.0, 6.0, ((0, 32),))
    out_grad = gaussian(key_list[1], (TOKENS, COLS), 1.0, 6.0, ((0, 32), (1, 16)))
    weight = gaussian(key_list[2], (DIN, COLS), DIN ** -0.5, 0.375, ((1, 16),), jnp.float32)
    error = gaussian(key_list[3], (REPLICAS, DIN, COLS), 1.0, 6.0, ((0, 32), (2, 16)), jnp.float32)
    start_q = gaussian(key_list[4], (COLS, RANK), COL_DEV ** -0.5, 0.1875, ((0, 16),), jnp.float32)
    return dict(acts=acts, out_grad=out_grad, weight=weight, error=error, start_q=start_q)


HIGH = lax.Precision.HIGHEST

def one_tile(carry, pieces):
    acts32, grads_t, error_t, weight_t, start_t = pieces
    grads32 = grads_t.astype(jnp.float32)
    gradient = jnp.einsum('rtd,rtc->rdc', acts32, grads32, precision=HIGH) / math.sqrt(TOK_DEV)
    merged = gradient + error_t
    left = lax.optimization_barrier(jnp.sum(jnp.einsum('rdc,ck->rdk', merged, start_t, precision=HIGH), axis=0)) / REPLICAS
    gram = jnp.dot(left.T, left, precision=HIGH)
    chol = jnp.linalg.cholesky(gram)
    ortho = jax.scipy.linalg.solve_triangular(chol, left.T, lower=True).T
    right = lax.optimization_barrier(jnp.sum(jnp.einsum('rdc,dk->rck', merged, ortho, precision=HIGH), axis=0)) / REPLICAS
    delta = jnp.dot(ortho, right.T, precision=HIGH)
    part = jnp.einsum('rtc,dc->rtd', grads32, weight_t, precision=HIGH)
    return (carry + part, (merged - delta[None], weight_t - delta))

def reference(acts, out_grad, weight, error, start_q):
    acts32 = acts.astype(jnp.float32).reshape(REPLICAS, TOK_DEV, DIN)
    grads = out_grad.reshape(REPLICAS, TOK_DEV, N_TENSOR, COL_DEV).transpose(2, 0, 1, 3)
    errors = error.reshape(REPLICAS, DIN, N_TENSOR, COL_DEV).transpose(2, 0, 1, 3)
    weights = weight.reshape(DIN, N_TENSOR, COL_DEV).transpose(1, 0, 2)
    starts = start_q.reshape(N_TENSOR, COL_DEV, RANK)
    init = jnp.zeros((REPLICAS, TOK_DEV, DIN), jnp.float32)

    def stepper(carry, items):
        return one_tile(carry, (acts32,) + items)
    total, outs = lax.scan(stepper, init, (grads, errors, weights, starts))
    new_errors, new_weights = outs
    new_error = new_errors.transpose(1, 2, 0, 3).reshape(REPLICAS, DIN, COLS)
    new_weight = new_weights.transpose(1, 0, 2).reshape(DIN, COLS)
    return (new_weight, new_error, total.reshape(TOKENS, DIN))
```

```python
import functools

import jax
import jax.numpy as jnp
from jax import lax
from jax.experimental import pallas as pl
from jax.experimental.pallas import tpu as pltpu
from jax.sharding import PartitionSpec as P

HIGH = lax.Precision.HIGHEST
F32 = jnp.float32
BF16 = jnp.bfloat16
NN = (((1,), (0,)), ((), ()))
NT = (((1,), (1,)), ((), ()))

NX, NY = 4, 8
NDP = NX * NY
NZ = 8

DIN, COL, TOK, RANK = 256, 1024, 1024, 64
BLK = 256
NB = COL // BLK
ROWS = TOK // (2 * NZ)
TILES = 16


def split(x):
    hi = x.astype(BF16)
    lo = (x - hi.astype(F32)).astype(BF16)
    return hi, lo


def dot(a, b, dims=NN):
    return lax.dot_general(a, b, dims, preferred_element_type=F32)


def spd_inverse(a):
    n = a.shape[0]
    rows = lax.broadcasted_iota(jnp.int32, (n, n), 0)
    cols = lax.broadcasted_iota(jnp.int32, (n, n), 1)
    lane = lax.broadcasted_iota(jnp.int32, (1, n), 1)

    def sweep(k, a):
        at_row, at_col = rows == k, cols == k
        row = jnp.sum(jnp.where(at_row, a, 0.0), axis=0, keepdims=True)
        col = jnp.sum(jnp.where(at_col, a, 0.0), axis=1, keepdims=True)
        pivot = jnp.sum(jnp.where(lane == k, row, 0.0), axis=1, keepdims=True)
        inv = 1.0 / pivot
        scaled = row * inv
        out = a - col * scaled
        out = jnp.where(at_col, col * inv, out)
        return jnp.where(at_row, jnp.where(lane == k, -inv, scaled), out)

    return -lax.fori_loop(0, n, sweep, a)


def mixed(i, n):
    return n // 2 + (2 * lax.rem(i + 1, 2) - 1) * ((i + 1) // 2)


def by_parity(i, parity):
    even = 4 + (1 - 2 * lax.rem(i, 2)) * 2 * ((i + 1) // 2)
    odd = 4 + (2 * lax.rem(i, 2) - 1) * (2 * (i // 2) + 1)
    return even + parity * (odd - even)


def comm_kernel(
    acts_h, og_h, w_h, err_h, q_h,
    merged, b4, s_all, ig,
    acts_v, og_v, w_v, err_v, q_v,
    acts_t, mhi, mlo, qt, w_hi, w_lo,
    l_send, l_recv, l_all, s_send, s_recv, part, p_recv, psum, z_recv,
    load_sem, send_l, recv_l, send_la, recv_la, send_s, recv_s, send_sa, recv_sa,
    send_p, recv_p, send_z, recv_z,
):
    me = lax.axis_index("dp")
    x, y = me // NY, lax.rem(me, NY)
    t = lax.axis_index("tensor")
    z, core = t // 2, lax.rem(t, 2)

    loads = [
        pltpu.make_async_copy(q_h, q_v, load_sem.at[0]),
        pltpu.make_async_copy(acts_h, acts_v, load_sem.at[1]),
    ]
    for n in range(NB):
        at = pl.ds(n * BLK, BLK)
        loads.append(pltpu.make_async_copy(og_h.at[:, at], og_v.at[:, at], load_sem.at[2 + n]))
        loads.append(
            pltpu.make_async_copy(err_h.at[:, at], err_v.at[:, at], load_sem.at[2 + NB + n])
        )
    loads.append(pltpu.make_async_copy(w_h, w_v, load_sem.at[2 + 2 * NB]))
    for load in loads:
        load.start()

    def at_offset(i):
        return lax.rem(x + mixed(lax.rem(i, NX), NX), NX) * NY + lax.rem(
            y + mixed(i // NX, NY), NY
        )

    barrier = pltpu.get_barrier_semaphore()

    def greet(i, _):
        pl.semaphore_signal(
            barrier, inc=1, device_id={"dp": at_offset(i)}, device_id_type=pl.DeviceIdType.MESH
        )
        return _

    lax.fori_loop(0, NDP - 1, greet, 0)

    def greet_z(i, _):
        peer = lax.rem(z + mixed(i, NZ), NZ) * 2 + core
        pl.semaphore_signal(
            barrier, inc=1, device_id={"tensor": peer}, device_id_type=pl.DeviceIdType.MESH
        )
        return _

    lax.fori_loop(0, NZ - 1, greet_z, 0)
    partner = z * 2 + 1 - core
    pl.semaphore_signal(
        barrier, inc=1, device_id={"tensor": partner}, device_id_type=pl.DeviceIdType.MESH
    )

    loads[0].wait()
    q_hi, q_lo = split(q_v[...].T)
    qt[0:RANK, :] = q_hi
    qt[RANK:, :] = q_lo
    loads[1].wait()
    acts_t[...] = acts_v[...].T
    for n in range(NB):
        at = pl.ds(n * BLK, BLK)
        loads[2 + 2 * n].wait()
        loads[3 + 2 * n].wait()
        m = dot(acts_t[...], og_v[:, at]) * (TOK ** -0.5) + err_v[:, at]
        merged[:, at] = m
        hi, lo = split(m)
        mhi[:, at] = hi
        mlo[:, at] = lo
    both = dot(qt[...], mhi[...], NT)
    left = both[0:RANK] + both[RANK:] + dot(qt[0:RANK, :], mlo[...], NT)
    l_send[0:8] = left[:, 0:128].reshape(8, 8, 128)
    l_send[8:16] = left[:, 128:256].reshape(8, 8, 128)

    pl.semaphore_wait(barrier, NDP - 1 + NZ - 1 + 1)

    my_tile = x * 4 + y // 2
    owner = lax.rem(x + y, 2) == 0

    def left_copy(peer, tile):
        return pltpu.make_async_remote_copy(
            src_ref=l_send.at[tile], dst_ref=l_recv.at[me], send_sem=send_l, recv_sem=recv_l,
            device_id={"dp": peer}, device_id_type=pl.DeviceIdType.MESH,
        )

    def left_to(i, _):
        dx = mixed(lax.rem(i, NX), NX)
        px = lax.rem(x + dx, NX)
        parity = lax.rem(x + y + dx, 2)
        py = lax.rem(y + by_parity(i // NX, parity), NY)
        peer = px * NY + py
        tile = px * 4 + py // 2

        @pl.when(peer != me)
        def _():
            left_copy(peer, tile).start()

        return _

    def skip(i, _):
        left_to(i, 0)
        return _

    lax.fori_loop(0, TILES, skip, 0)

    @pl.when(owner)
    def _():
        l_recv[me] = l_send[my_tile]

    loads[2 + 2 * NB].wait()
    wh, wl = split(w_v[...])
    w_hi[...] = wh
    w_lo[...] = wl

    def part_rows(i, _):
        rows = og_v[pl.ds(pl.multiple_of(i * 256, 256), 256), :]
        p = dot(rows, w_hi[...], NT) + dot(rows, w_lo[...], NT)
        p = p.reshape(2, 2, ROWS, DIN)
        for c in range(2):
            for half in range(2):
                part[c, 2 * i + half] = p[half, c]
        return _

    lax.fori_loop(0, TOK // 256, part_rows, 0)
    to_partner = pltpu.make_async_remote_copy(
        src_ref=part.at[1 - core], dst_ref=p_recv, send_sem=send_p, recv_sem=recv_p,
        device_id={"tensor": partner}, device_id_type=pl.DeviceIdType.MESH,
    )
    to_partner.start()

    def left_all(peer):
        return pltpu.make_async_remote_copy(
            src_ref=l_all.at[my_tile], dst_ref=l_all.at[my_tile], send_sem=send_la,
            recv_sem=recv_la, device_id={"dp": peer}, device_id_type=pl.DeviceIdType.MESH,
        )

    @pl.when(owner)
    def _():
        pltpu.make_async_copy(
            l_recv.at[pl.ds(0, NDP - 1)], l_recv.at[pl.ds(0, NDP - 1)], recv_l
        ).wait()
        l_all[my_tile] = jnp.sum(l_recv[...], axis=0) * (1.0 / NDP)

        def to(i, _):
            left_all(at_offset(i)).start()
            return _

        lax.fori_loop(0, NDP - 1, to, 0)

    to_partner.wait_recv()

    def pair_sum(i, _):
        psum[i] = part[core, i] + p_recv[i]
        return _

    lax.fori_loop(0, NZ, pair_sum, 0)

    def z_copy(pz):
        return pltpu.make_async_remote_copy(
            src_ref=psum.at[pz], dst_ref=z_recv.at[z], send_sem=send_z, recv_sem=recv_z,
            device_id={"tensor": pz * 2 + core}, device_id_type=pl.DeviceIdType.MESH,
        )

    def z_to(i, _):
        z_copy(lax.rem(z + mixed(i, NZ), NZ)).start()
        return _

    lax.fori_loop(0, NZ - 1, z_to, 0)
    z_recv[z] = psum[z]

    @pl.when(owner)
    def _():
        pltpu.make_async_copy(
            l_all.at[pl.ds(0, TILES - 1)], l_all.at[pl.ds(0, TILES - 1)], recv_la
        ).wait()

    @pl.when(jnp.logical_not(owner))
    def _():
        pltpu.make_async_copy(l_all, l_all, recv_la).wait()

    left = jnp.concatenate(
        [l_all[0:8].reshape(RANK, 128), l_all[8:16].reshape(RANK, 128)], axis=1
    )
    l_hi, l_lo = split(left)
    l_both = jnp.concatenate([l_hi, l_lo], axis=0)
    for n in range(NB):
        at = pl.ds(n * BLK, BLK)
        both = dot(l_both, mhi[:, at])
        s = both[0:RANK] + both[RANK:] + dot(l_hi, mlo[:, at])
        s_send[8 * n : 8 * n + 8] = s.reshape(8, 8, BLK)

    def s_to(i, _):
        peer = at_offset(i)
        pltpu.make_async_remote_copy(
            src_ref=s_send.at[peer], dst_ref=s_recv.at[me], send_sem=send_s, recv_sem=recv_s,
            device_id={"dp": peer}, device_id_type=pl.DeviceIdType.MESH,
        ).start()
        return _

    lax.fori_loop(0, NDP - 1, s_to, 0)
    s_recv[me] = s_send[me]

    gram = lax.dot_general(left, left, NT, precision=HIGH, preferred_element_type=F32)
    inv = spd_inverse(gram)
    bt = lax.dot_general(inv, left, NN, precision=HIGH, preferred_element_type=F32)
    b_hi, b_lo = split(bt.T * (1.0 / NDP))
    b4[...] = jnp.concatenate([b_hi, b_hi, b_lo, b_lo], axis=1)

    pltpu.make_async_copy(
        s_recv.at[pl.ds(0, NDP - 1)], s_recv.at[pl.ds(0, NDP - 1)], recv_s
    ).wait()
    s_all[me] = jnp.sum(s_recv[...], axis=0)

    def s_all_to(i, _):
        pltpu.make_async_remote_copy(
            src_ref=s_all.at[me], dst_ref=s_all.at[me], send_sem=send_sa, recv_sem=recv_sa,
            device_id={"dp": at_offset(i)}, device_id_type=pl.DeviceIdType.MESH,
        ).start()
        return _

    lax.fori_loop(0, NDP - 1, s_all_to, 0)

    pltpu.make_async_copy(
        z_recv.at[pl.ds(0, NZ - 1)], z_recv.at[pl.ds(0, NZ - 1)], recv_z
    ).wait()
    ig[...] = jnp.sum(z_recv[...], axis=0)

    to_partner.wait_send()
    pltpu.make_async_copy(psum.at[pl.ds(0, NZ - 1)], psum.at[pl.ds(0, NZ - 1)], send_z).wait()

    @pl.when(owner)
    def _():
        pltpu.make_async_copy(
            l_send.at[pl.ds(0, TILES - 1)], l_send.at[pl.ds(0, TILES - 1)], send_l
        ).wait()
        pltpu.make_async_copy(
            l_recv.at[pl.ds(0, NDP - 1)], l_recv.at[pl.ds(0, NDP - 1)], send_la
        ).wait()

    @pl.when(jnp.logical_not(owner))
    def _():
        pltpu.make_async_copy(l_send, l_send, send_l).wait()

    for sem in (send_s, send_sa, recv_sa):
        pltpu.make_async_copy(
            s_send.at[pl.ds(0, NDP - 1)], s_send.at[pl.ds(0, NDP - 1)], sem
        ).wait()


def finish_kernel(merged, b4, s_all, w, ig_in, new_w, new_e, ig):
    s_hi, s_lo = split(s_all[...].reshape(RANK, BLK))
    delta = dot(b4[...], jnp.concatenate([s_hi, s_lo, s_hi, s_lo], axis=0))
    new_e[...] = merged[...] - delta
    new_w[...] = w[...] - delta

    @pl.when(pl.program_id(0) == 0)
    def _():
        ig[...] = ig_in[...]


def local(acts, out_grad, weight, error, start_q):
    hbm = pl.BlockSpec(memory_space=pl.ANY)
    vmem = pl.BlockSpec(memory_space=pltpu.VMEM)
    shape = jax.ShapeDtypeStruct
    dma = pltpu.SemaphoreType.DMA
    merged, b4, s_all, ig = pl.pallas_call(
        comm_kernel,
        out_shape=(
            shape((DIN, COL), F32),
            shape((DIN, 4 * RANK), BF16),
            shape((NDP, 8, BLK), F32),
            shape((ROWS, DIN), F32),
        ),
        in_specs=[hbm] * 5,
        out_specs=(vmem,) * 4,
        scratch_shapes=[
            pltpu.VMEM((TOK, DIN), BF16),
            pltpu.VMEM((TOK, COL), BF16),
            pltpu.VMEM((DIN, COL), F32),
            pltpu.VMEM((DIN, COL), F32),
            pltpu.VMEM((COL, RANK), F32),
            pltpu.VMEM((DIN, TOK), BF16),
            pltpu.VMEM((DIN, COL), BF16),
            pltpu.VMEM((DIN, COL), BF16),
            pltpu.VMEM((2 * RANK, COL), BF16),
            pltpu.VMEM((DIN, COL), BF16),
            pltpu.VMEM((DIN, COL), BF16),
            pltpu.VMEM((TILES, 8, 128), F32),
            pltpu.VMEM((NDP, 8, 128), F32),
            pltpu.VMEM((TILES, 8, 128), F32),
            pltpu.VMEM((NDP, 8, BLK), F32),
            pltpu.VMEM((NDP, 8, BLK), F32),
            pltpu.VMEM((2, NZ, ROWS, DIN), F32),
            pltpu.VMEM((NZ, ROWS, DIN), F32),
            pltpu.VMEM((NZ, ROWS, DIN), F32),
            pltpu.VMEM((NZ, ROWS, DIN), F32),
            dma((3 + 2 * NB,)),
        ]
        + [dma] * 12,
        compiler_params=pltpu.CompilerParams(
            collective_id=0, has_side_effects=True, vmem_limit_bytes=40 * 1024 * 1024
        ),
        name="powersgd_comm",
    )(acts, out_grad, weight, error[0], start_q)
    block = pl.BlockSpec((DIN, BLK), lambda n: (0, n))
    whole = pl.BlockSpec((ROWS, DIN), lambda n: (0, 0))
    new_weight, new_error, input_grad = pl.pallas_call(
        finish_kernel,
        grid=(NB,),
        out_shape=(shape((DIN, COL), F32), shape((DIN, COL), F32), shape((ROWS, DIN), F32)),
        in_specs=[
            block,
            pl.BlockSpec((DIN, 4 * RANK), lambda n: (0, 0)),
            pl.BlockSpec((8, 8, BLK), lambda n: (n, 0, 0)),
            block,
            whole,
        ],
        out_specs=(block, block, whole),
        name="powersgd_finish",
    )(merged, b4, s_all, weight, ig)
    return new_weight, new_error[None], input_grad


def solution(mesh):
    placed = (
        P("dp", None),
        P("dp", "tensor"),
        P(None, "tensor"),
        P("dp", None, "tensor"),
        P("tensor", None),
    )
    return jax.shard_map(
        local,
        mesh=mesh,
        in_specs=placed,
        out_specs=(P(None, "tensor"), P("dp", None, "tensor"), P(("dp", "tensor"), None)),
        check_vma=False,
    )
```

```python
import functools

import jax
import jax.numpy as jnp
from jax import lax
from jax.experimental import pallas as pl
from jax.experimental.pallas import tpu as pltpu
from jax.sharding import PartitionSpec as P

HIGH = lax.Precision.HIGHEST
F32 = jnp.float32
BF16 = jnp.bfloat16
NN = (((1,), (0,)), ((), ()))
NT = (((1,), (1,)), ((), ()))

NX, NY = 4, 8
NDP = NX * NY
NZ = 8

DIN, COL, TOK, RANK = 256, 1024, 1024, 64
BLK = 256
NB = COL // BLK
ROWS = TOK // (2 * NZ)
TILES = 16


def split(x):
    hi = x.astype(BF16)
    lo = (x - hi.astype(F32)).astype(BF16)
    return hi, lo


def dot(a, b, dims=NN):
    return lax.dot_general(a, b, dims, preferred_element_type=F32)


def spd_inverse(a):
    n = a.shape[0]
    rows = lax.broadcasted_iota(jnp.int32, (n, n), 0)
    cols = lax.broadcasted_iota(jnp.int32, (n, n), 1)
    lane = lax.broadcasted_iota(jnp.int32, (1, n), 1)

    def sweep(k, a):
        at_row, at_col = rows == k, cols == k
        row = jnp.sum(jnp.where(at_row, a, 0.0), axis=0, keepdims=True)
        col = jnp.sum(jnp.where(at_col, a, 0.0), axis=1, keepdims=True)
        pivot = jnp.sum(jnp.where(lane == k, row, 0.0), axis=1, keepdims=True)
        inv = 1.0 / pivot
        scaled = row * inv
        out = a - col * scaled
        out = jnp.where(at_col, col * inv, out)
        return jnp.where(at_row, jnp.where(lane == k, -inv, scaled), out)

    return -lax.fori_loop(0, n, sweep, a)


def mixed(i, n):
    return n // 2 + (2 * lax.rem(i + 1, 2) - 1) * ((i + 1) // 2)


def by_parity(i, parity):
    even = 4 + (1 - 2 * lax.rem(i, 2)) * 2 * ((i + 1) // 2)
    odd = 4 + (2 * lax.rem(i, 2) - 1) * (2 * (i // 2) + 1)
    return even + parity * (odd - even)


def comm_kernel(
    acts_h, og_h, w_h, err_h, q_h,
    merged, b4, s_all, ig, w_v,
    acts_v, og_v, err_v, q_v,
    acts_t, mhi, mlo, qt, w_hi, w_lo,
    l_send, l_recv, l_all, s_send, s_recv, part, p_recv, psum, z_recv,
    load_sem, send_l, recv_l, send_la, recv_la, send_s, recv_s, send_sa, recv_sa,
    send_p, recv_p, send_z, recv_z,
):
    me = lax.axis_index("dp")
    x, y = me // NY, lax.rem(me, NY)
    t = lax.axis_index("tensor")
    z, core = t // 2, lax.rem(t, 2)

    loads = [
        pltpu.make_async_copy(q_h, q_v, load_sem.at[0]),
        pltpu.make_async_copy(acts_h, acts_v, load_sem.at[1]),
    ]
    for n in range(NB):
        at = pl.ds(n * BLK, BLK)
        loads.append(pltpu.make_async_copy(og_h.at[:, at], og_v.at[:, at], load_sem.at[2 + n]))
        loads.append(
            pltpu.make_async_copy(err_h.at[:, at], err_v.at[:, at], load_sem.at[2 + NB + n])
        )
    loads.append(pltpu.make_async_copy(w_h, w_v, load_sem.at[2 + 2 * NB]))
    for load in loads:
        load.start()

    def at_offset(i):
        return lax.rem(x + mixed(lax.rem(i, NX), NX), NX) * NY + lax.rem(
            y + mixed(i // NX, NY), NY
        )

    barrier = pltpu.get_barrier_semaphore()

    def greet(i, _):
        pl.semaphore_signal(
            barrier, inc=1, device_id={"dp": at_offset(i)}, device_id_type=pl.DeviceIdType.MESH
        )
        return _

    lax.fori_loop(0, NDP - 1, greet, 0)

    def greet_z(i, _):
        peer = lax.rem(z + mixed(i, NZ), NZ) * 2 + core
        pl.semaphore_signal(
            barrier, inc=1, device_id={"tensor": peer}, device_id_type=pl.DeviceIdType.MESH
        )
        return _

    lax.fori_loop(0, NZ - 1, greet_z, 0)
    partner = z * 2 + 1 - core
    pl.semaphore_signal(
        barrier, inc=1, device_id={"tensor": partner}, device_id_type=pl.DeviceIdType.MESH
    )

    loads[0].wait()
    q_hi, q_lo = split(q_v[...])
    qt[0:RANK, :] = q_hi
    qt[RANK:, :] = q_lo
    loads[1].wait()
    acts_t[...] = acts_v[...].T
    for n in range(NB):
        at = pl.ds(n * BLK, BLK)
        loads[2 + 2 * n].wait()
        loads[3 + 2 * n].wait()
        m = dot(acts_t[...], og_v[:, at]) * (TOK ** -0.5) + err_v[:, at]
        merged[:, at] = m
        hi, lo = split(m)
        mhi[:, at] = hi
        mlo[:, at] = lo
    both = dot(qt[...], mhi[...], NT)
    left = both[0:RANK] + both[RANK:] + dot(qt[0:RANK, :], mlo[...], NT)
    l_send[0:8] = left[:, 0:128].reshape(8, 8, 128)
    l_send[8:16] = left[:, 128:256].reshape(8, 8, 128)

    pl.semaphore_wait(barrier, NDP - 1 + NZ - 1 + 1)

    my_tile = x * 4 + y // 2
    owner = lax.rem(x + y, 2) == 0

    def left_copy(peer, tile):
        return pltpu.make_async_remote_copy(
            src_ref=l_send.at[tile], dst_ref=l_recv.at[me], send_sem=send_l, recv_sem=recv_l,
            device_id={"dp": peer}, device_id_type=pl.DeviceIdType.MESH,
        )

    def left_to(i, _):
        dx = mixed(lax.rem(i, NX), NX)
        px = lax.rem(x + dx, NX)
        parity = lax.rem(x + y + dx, 2)
        py = lax.rem(y + by_parity(i // NX, parity), NY)
        peer = px * NY + py
        tile = px * 4 + py // 2

        @pl.when(peer != me)
        def _():
            left_copy(peer, tile).start()

        return _

    def skip(i, _):
        left_to(i, 0)
        return _

    lax.fori_loop(0, TILES, skip, 0)

    @pl.when(owner)
    def _():
        l_recv[me] = l_send[my_tile]

    loads[2 + 2 * NB].wait()
    wh, wl = split(w_v[...])
    w_hi[...] = wh
    w_lo[...] = wl

    def part_rows(i, _):
        rows = og_v[pl.ds(pl.multiple_of(i * 256, 256), 256), :]
        p = dot(rows, w_hi[...], NT) + dot(rows, w_lo[...], NT)
        p = p.reshape(2, 2, ROWS, DIN)
        for c in range(2):
            for half in range(2):
                part[c, 2 * i + half] = p[half, c]
        return _

    lax.fori_loop(0, TOK // 256, part_rows, 0)
    to_partner = pltpu.make_async_remote_copy(
        src_ref=part.at[1 - core], dst_ref=p_recv, send_sem=send_p, recv_sem=recv_p,
        device_id={"tensor": partner}, device_id_type=pl.DeviceIdType.MESH,
    )
    to_partner.start()

    def left_all(peer):
        return pltpu.make_async_remote_copy(
            src_ref=l_all.at[my_tile], dst_ref=l_all.at[my_tile], send_sem=send_la,
            recv_sem=recv_la, device_id={"dp": peer}, device_id_type=pl.DeviceIdType.MESH,
        )

    @pl.when(owner)
    def _():
        pltpu.make_async_copy(
            l_recv.at[pl.ds(0, NDP - 1)], l_recv.at[pl.ds(0, NDP - 1)], recv_l
        ).wait()
        l_all[my_tile] = jnp.sum(l_recv[...], axis=0) * (1.0 / NDP)

        def to(i, _):
            left_all(at_offset(i)).start()
            return _

        lax.fori_loop(0, NDP - 1, to, 0)

    to_partner.wait_recv()

    def pair_sum(i, _):
        psum[i] = part[core, i] + p_recv[i]
        return _

    lax.fori_loop(0, NZ, pair_sum, 0)

    def z_copy(pz):
        return pltpu.make_async_remote_copy(
            src_ref=psum.at[pz], dst_ref=z_recv.at[z], send_sem=send_z, recv_sem=recv_z,
            device_id={"tensor": pz * 2 + core}, device_id_type=pl.DeviceIdType.MESH,
        )

    def z_to(i, _):
        z_copy(lax.rem(z + mixed(i, NZ), NZ)).start()
        return _

    lax.fori_loop(0, NZ - 1, z_to, 0)
    z_recv[z] = psum[z]

    @pl.when(owner)
    def _():
        pltpu.make_async_copy(
            l_all.at[pl.ds(0, TILES - 1)], l_all.at[pl.ds(0, TILES - 1)], recv_la
        ).wait()

    @pl.when(jnp.logical_not(owner))
    def _():
        pltpu.make_async_copy(l_all, l_all, recv_la).wait()

    left = jnp.concatenate(
        [l_all[0:8].reshape(RANK, 128), l_all[8:16].reshape(RANK, 128)], axis=1
    )
    l_hi, l_lo = split(left)
    l_both = jnp.concatenate([l_hi, l_lo], axis=0)
    for n in range(NB):
        at = pl.ds(n * BLK, BLK)
        both = dot(l_both, mhi[:, at])
        s = both[0:RANK] + both[RANK:] + dot(l_hi, mlo[:, at])
        s_send[8 * n : 8 * n + 8] = s.reshape(8, 8, BLK)

    def s_to(i, _):
        peer = at_offset(i)
        pltpu.make_async_remote_copy(
            src_ref=s_send.at[peer], dst_ref=s_recv.at[me], send_sem=send_s, recv_sem=recv_s,
            device_id={"dp": peer}, device_id_type=pl.DeviceIdType.MESH,
        ).start()
        return _

    lax.fori_loop(0, NDP - 1, s_to, 0)
    s_recv[me] = s_send[me]

    gram = lax.dot_general(left, left, NT, precision=HIGH, preferred_element_type=F32)
    inv = spd_inverse(gram)
    bt = lax.dot_general(inv, left, NN, precision=HIGH, preferred_element_type=F32)
    b_hi, b_lo = split(bt.T * (1.0 / NDP))
    b4[...] = jnp.concatenate([b_hi, b_hi, b_lo, b_lo], axis=1)

    pltpu.make_async_copy(
        s_recv.at[pl.ds(0, NDP - 1)], s_recv.at[pl.ds(0, NDP - 1)], recv_s
    ).wait()
    s_all[me] = jnp.sum(s_recv[...], axis=0)

    def s_all_to(i, _):
        pltpu.make_async_remote_copy(
            src_ref=s_all.at[me], dst_ref=s_all.at[me], send_sem=send_sa, recv_sem=recv_sa,
            device_id={"dp": at_offset(i)}, device_id_type=pl.DeviceIdType.MESH,
        ).start()
        return _

    lax.fori_loop(0, NDP - 1, s_all_to, 0)

    pltpu.make_async_copy(
        z_recv.at[pl.ds(0, NZ - 1)], z_recv.at[pl.ds(0, NZ - 1)], recv_z
    ).wait()
    ig[...] = jnp.sum(z_recv[...], axis=0)

    to_partner.wait_send()
    pltpu.make_async_copy(psum.at[pl.ds(0, NZ - 1)], psum.at[pl.ds(0, NZ - 1)], send_z).wait()

    @pl.when(owner)
    def _():
        pltpu.make_async_copy(
            l_send.at[pl.ds(0, TILES - 1)], l_send.at[pl.ds(0, TILES - 1)], send_l
        ).wait()
        pltpu.make_async_copy(
            l_recv.at[pl.ds(0, NDP - 1)], l_recv.at[pl.ds(0, NDP - 1)], send_la
        ).wait()

    @pl.when(jnp.logical_not(owner))
    def _():
        pltpu.make_async_copy(l_send, l_send, send_l).wait()

    for sem in (send_s, send_sa, recv_sa):
        pltpu.make_async_copy(
            s_send.at[pl.ds(0, NDP - 1)], s_send.at[pl.ds(0, NDP - 1)], sem
        ).wait()


def finish_kernel(merged, b4, s_all, w, ig_in, new_w, new_e, ig, w_v, e_v, out_sem):
    copies = [pltpu.make_async_copy(ig_in, ig, out_sem.at[0])]
    copies[0].start()
    for n in range(NB):
        at = pl.ds(n * BLK, BLK)
        s_hi, s_lo = split(s_all[8 * n : 8 * n + 8].reshape(RANK, BLK))
        delta = dot(b4[...], jnp.concatenate([s_hi, s_lo, s_hi, s_lo], axis=0))
        e_v[:, at] = merged[:, at] - delta
        w_v[:, at] = w[:, at] - delta
        for i, (src, dst) in enumerate(((e_v, new_e), (w_v, new_w))):
            copies.append(
                pltpu.make_async_copy(src.at[:, at], dst.at[:, at], out_sem.at[1 + 2 * n + i])
            )
            copies[-1].start()
    for copy in copies:
        copy.wait()


def local(acts, out_grad, weight, error, start_q):
    hbm = pl.BlockSpec(memory_space=pltpu.HBM)
    vmem = pl.BlockSpec(memory_space=pltpu.VMEM)
    shape = jax.ShapeDtypeStruct
    dma = pltpu.SemaphoreType.DMA
    merged, b4, s_all, ig, weight_v = pl.pallas_call(
        comm_kernel,
        out_shape=(
            shape((DIN, COL), F32),
            shape((DIN, 4 * RANK), BF16),
            shape((NDP, 8, BLK), F32),
            shape((ROWS, DIN), F32),
            shape((DIN, COL), F32),
        ),
        in_specs=[hbm] * 5,
        out_specs=(vmem,) * 5,
        scratch_shapes=[
            pltpu.VMEM((TOK, DIN), BF16),
            pltpu.VMEM((TOK, COL), BF16),
            pltpu.VMEM((DIN, COL), F32),
            pltpu.VMEM((RANK, COL), F32),
            pltpu.VMEM((DIN, TOK), BF16),
            pltpu.VMEM((DIN, COL), BF16),
            pltpu.VMEM((DIN, COL), BF16),
            pltpu.VMEM((2 * RANK, COL), BF16),
            pltpu.VMEM((DIN, COL), BF16),
            pltpu.VMEM((DIN, COL), BF16),
            pltpu.VMEM((TILES, 8, 128), F32),
            pltpu.VMEM((NDP, 8, 128), F32),
            pltpu.VMEM((TILES, 8, 128), F32),
            pltpu.VMEM((NDP, 8, BLK), F32),
            pltpu.VMEM((NDP, 8, BLK), F32),
            pltpu.VMEM((2, NZ, ROWS, DIN), F32),
            pltpu.VMEM((NZ, ROWS, DIN), F32),
            pltpu.VMEM((NZ, ROWS, DIN), F32),
            pltpu.VMEM((NZ, ROWS, DIN), F32),
            dma((3 + 2 * NB,)),
        ]
        + [dma] * 12,
        compiler_params=pltpu.CompilerParams(
            collective_id=0, has_side_effects=True, vmem_limit_bytes=40 * 1024 * 1024
        ),
        name="powersgd_comm",
    )(*(pltpu.with_memory_space_constraint(a, pltpu.HBM) for a in (acts, out_grad, weight, error[0], start_q.T)))
    new_weight, new_error, input_grad = pl.pallas_call(
        finish_kernel,
        out_shape=(shape((DIN, COL), F32), shape((DIN, COL), F32), shape((ROWS, DIN), F32)),
        in_specs=[vmem] * 5,
        out_specs=(hbm,) * 3,
        scratch_shapes=[
            pltpu.VMEM((DIN, COL), F32),
            pltpu.VMEM((DIN, COL), F32),
            dma((1 + 2 * NB,)),
        ],
        compiler_params=pltpu.CompilerParams(vmem_limit_bytes=16 * 1024 * 1024),
        name="powersgd_finish",
    )(merged, b4, s_all, weight_v, ig)
    return new_weight, new_error[None], input_grad


def solution(mesh):
    placed = (
        P("dp", None),
        P("dp", "tensor"),
        P(None, "tensor"),
        P("dp", None, "tensor"),
        P("tensor", None),
    )
    return jax.shard_map(
        local,
        mesh=mesh,
        in_specs=placed,
        out_specs=(P(None, "tensor"), P("dp", None, "tensor"), P(("dp", "tensor"), None)),
        check_vma=False,
    )
```

```python
import functools

import jax
import jax.numpy as jnp
from jax import lax
from jax.experimental import pallas as pl
from jax.experimental.pallas import tpu as pltpu
from jax.sharding import PartitionSpec as P

HIGH = lax.Precision.HIGHEST
F32 = jnp.float32
BF16 = jnp.bfloat16
NN = (((1,), (0,)), ((), ()))
NT = (((1,), (1,)), ((), ()))

NX, NY = 4, 8
NDP = NX * NY
NZ = 8

DIN, COL, TOK, RANK = 256, 1024, 1024, 64
BLK = 256
NB = COL // BLK
ROWS = TOK // (2 * NZ)
TILES = 16


def split(x):
    hi = x.astype(BF16)
    lo = (x - hi.astype(F32)).astype(BF16)
    return hi, lo


def dot(a, b, dims=NN):
    return lax.dot_general(a, b, dims, preferred_element_type=F32)


def sweeps(a, start, stop):
    n = a.shape[0]
    rows = lax.broadcasted_iota(jnp.int32, (n, n), 0)
    cols = lax.broadcasted_iota(jnp.int32, (n, n), 1)
    lane = lax.broadcasted_iota(jnp.int32, (1, n), 1)

    def sweep(k, a):
        at_row, at_col = rows == k, cols == k
        row = jnp.sum(jnp.where(at_row, a, 0.0), axis=0, keepdims=True)
        col = jnp.sum(jnp.where(at_col, a, 0.0), axis=1, keepdims=True)
        pivot = jnp.sum(jnp.where(lane == k, row, 0.0), axis=1, keepdims=True)
        inv = 1.0 / pivot
        scaled = row * inv
        out = a - col * scaled
        out = jnp.where(at_col, col * inv, out)
        return jnp.where(at_row, jnp.where(lane == k, -inv, scaled), out)

    return lax.fori_loop(start, stop, sweep, a)


FAR_X = (2, 1, 3, 0)
FAR_Y = (4, 3, 5, 2, 6, 1, 7, 0)
FAR_EVEN, FAR_ODD = (4, 2, 6, 0), (3, 5, 1, 7)
HALF = 36


def comm_kernel(
    acts_h, og_h, w_h, err_h, q_h,
    merged, b4, s_all, ig, w_v,
    acts_v, og_v, err_v, q_v,
    acts_t, mhi, mlo, qt, w_hi, w_lo,
    l_send, l_recv, l_all, s_send, s_recv, part, p_recv, psum, z_recv,
    load_sem, send_l, recv_l, send_la, recv_la, send_s, recv_s, send_sa, recv_sa,
    send_p, recv_p, send_z, recv_z,
):
    me = lax.axis_index("dp")
    x, y = me // NY, lax.rem(me, NY)
    t = lax.axis_index("tensor")
    z, core = t // 2, lax.rem(t, 2)

    loads = [
        pltpu.make_async_copy(q_h, q_v, load_sem.at[0]),
        pltpu.make_async_copy(acts_h, acts_v, load_sem.at[1]),
    ]
    for n in range(NB):
        at = pl.ds(n * BLK, BLK)
        loads.append(pltpu.make_async_copy(og_h.at[:, at], og_v.at[:, at], load_sem.at[2 + n]))
        loads.append(
            pltpu.make_async_copy(err_h.at[:, at], err_v.at[:, at], load_sem.at[2 + NB + n])
        )
    loads.append(pltpu.make_async_copy(w_h, w_v, load_sem.at[2 + 2 * NB]))
    for load in loads:
        load.start()

    xs = [lax.rem(x + d, NX) if d else x for d in FAR_X]
    ys = [lax.rem(y + d, NY) if d else y for d in FAR_Y]
    zs = [lax.rem(z + d, NZ) for d in FAR_Y[:-1]]
    peers = [px * NY + py for py in ys for px in xs][:-1]
    partner = z * 2 + 1 - core

    barrier = pltpu.get_barrier_semaphore()
    met = [{"dp": p} for p in peers] + [{"tensor": pz * 2 + core} for pz in zs]
    met.append({"tensor": partner})
    for device in met:
        pl.semaphore_signal(
            barrier, inc=1, device_id=device, device_id_type=pl.DeviceIdType.MESH
        )

    loads[0].wait()
    q_hi, q_lo = split(q_v[...])
    qt[0:RANK, :] = q_hi
    qt[RANK:, :] = q_lo
    loads[1].wait()
    acts_t[...] = acts_v[...].T
    both = jnp.zeros((2 * RANK, DIN), F32)
    left = jnp.zeros((RANK, DIN), F32)
    for n in range(NB):
        at = pl.ds(n * BLK, BLK)
        loads[2 + 2 * n].wait()
        loads[3 + 2 * n].wait()
        m = dot(acts_t[...], og_v[:, at]) * (TOK ** -0.5) + err_v[:, at]
        merged[:, at] = m
        hi, lo = split(m)
        mhi[:, at] = hi
        mlo[:, at] = lo
        both += dot(qt[:, at], hi, NT)
        left += dot(qt[0:RANK, at], lo, NT)
    left += both[0:RANK] + both[RANK:]
    l_send[0:8] = left[:, 0:128].reshape(8, 8, 128)
    l_send[8:16] = left[:, 128:256].reshape(8, 8, 128)

    pl.semaphore_wait(barrier, len(met))

    my_tile = x * 4 + y // 2
    owner = lax.rem(x + y, 2) == 0

    def left_copy(peer, tile):
        return pltpu.make_async_remote_copy(
            src_ref=l_send.at[tile], dst_ref=l_recv.at[me], send_sem=send_l, recv_sem=recv_l,
            device_id={"dp": peer}, device_id_type=pl.DeviceIdType.MESH,
        )

    odd = lax.rem(x + y, 2)
    same = [lax.rem(y + e + odd * (o - e), NY) for e, o in zip(FAR_EVEN, FAR_ODD)]
    other = [lax.rem(y + o + odd * (e - o), NY) for e, o in zip(FAR_EVEN, FAR_ODD)]
    for j in range(4):
        for dx, px in zip(FAR_X, xs):
            py = (other if dx % 2 else same)[j]
            copy = left_copy(px * NY + py, px * 4 + py // 2)
            if dx == 0 and j == 3:
                pl.when(jnp.logical_not(owner))(copy.start)
            else:
                copy.start()

    @pl.when(owner)
    def _():
        l_recv[me] = l_send[my_tile]

    loads[2 + 2 * NB].wait()
    wh, wl = split(w_v[...])
    w_hi[...] = wh
    w_lo[...] = wl

    def part_rows(i, _):
        rows = og_v[pl.ds(pl.multiple_of(i * 256, 256), 256), :]
        p = dot(rows, w_hi[...], NT) + dot(rows, w_lo[...], NT)
        p = p.reshape(2, 2, ROWS, DIN)
        for c in range(2):
            for half in range(2):
                part[c, 2 * i + half] = p[half, c]
        return _

    lax.fori_loop(0, TOK // 256, part_rows, 0)
    to_partner = pltpu.make_async_remote_copy(
        src_ref=part.at[1 - core], dst_ref=p_recv, send_sem=send_p, recv_sem=recv_p,
        device_id={"tensor": partner}, device_id_type=pl.DeviceIdType.MESH,
    )
    to_partner.start()

    def left_all(peer):
        return pltpu.make_async_remote_copy(
            src_ref=l_all.at[my_tile], dst_ref=l_all.at[my_tile], send_sem=send_la,
            recv_sem=recv_la, device_id={"dp": peer}, device_id_type=pl.DeviceIdType.MESH,
        )

    @pl.when(owner)
    def _():
        pltpu.make_async_copy(
            l_recv.at[pl.ds(0, NDP - 1)], l_recv.at[pl.ds(0, NDP - 1)], recv_l
        ).wait()
        l_all[my_tile] = jnp.sum(l_recv[...], axis=0) * (1.0 / NDP)

        for peer in peers:
            left_all(peer).start()

    to_partner.wait_recv()

    def pair_sum(i, _):
        psum[i] = part[core, i] + p_recv[i]
        return _

    lax.fori_loop(0, NZ, pair_sum, 0)

    def z_copy(pz):
        return pltpu.make_async_remote_copy(
            src_ref=psum.at[pz], dst_ref=z_recv.at[z], send_sem=send_z, recv_sem=recv_z,
            device_id={"tensor": pz * 2 + core}, device_id_type=pl.DeviceIdType.MESH,
        )

    for pz in zs:
        z_copy(pz).start()
    z_recv[z] = psum[z]

    @pl.when(owner)
    def _():
        pltpu.make_async_copy(
            l_all.at[pl.ds(0, TILES - 1)], l_all.at[pl.ds(0, TILES - 1)], recv_la
        ).wait()

    @pl.when(jnp.logical_not(owner))
    def _():
        pltpu.make_async_copy(l_all, l_all, recv_la).wait()

    left = jnp.concatenate(
        [l_all[0:8].reshape(RANK, 128), l_all[8:16].reshape(RANK, 128)], axis=1
    )
    l_hi, l_lo = split(left)
    l_both = jnp.concatenate([l_hi, l_lo], axis=0)
    for dx, px in zip(FAR_X, xs):
        at = pl.ds(pl.multiple_of(px * BLK, BLK), BLK)
        both = dot(l_both, mhi[:, at])
        s = both[0:RANK] + both[RANK:] + dot(l_hi, mlo[:, at])
        s_send[pl.ds(px * NY, NY)] = s.reshape(NY, 8, BLK)
        for dy, py in zip(FAR_Y, ys):
            if dx or dy:
                peer = px * NY + py
                pltpu.make_async_remote_copy(
                    src_ref=s_send.at[peer], dst_ref=s_recv.at[me], send_sem=send_s,
                    recv_sem=recv_s, device_id={"dp": peer},
                    device_id_type=pl.DeviceIdType.MESH,
                ).start()
    s_recv[me] = s_send[me]

    gram = lax.dot_general(left, left, NT, precision=HIGH, preferred_element_type=F32)
    swept = sweeps(gram, 0, HALF)

    pltpu.make_async_copy(
        s_recv.at[pl.ds(0, NDP - 1)], s_recv.at[pl.ds(0, NDP - 1)], recv_s
    ).wait()
    s_all[me] = jnp.sum(s_recv[...], axis=0)

    for peer in peers:
        pltpu.make_async_remote_copy(
            src_ref=s_all.at[me], dst_ref=s_all.at[me], send_sem=send_sa, recv_sem=recv_sa,
            device_id={"dp": peer}, device_id_type=pl.DeviceIdType.MESH,
        ).start()

    inv = -sweeps(swept, HALF, RANK)
    bt = lax.dot_general(inv, left, NN, precision=HIGH, preferred_element_type=F32)
    b_hi, b_lo = split(bt.T * (1.0 / NDP))
    b4[...] = jnp.concatenate([b_hi, b_hi, b_lo, b_lo], axis=1)

    pltpu.make_async_copy(
        z_recv.at[pl.ds(0, NZ - 1)], z_recv.at[pl.ds(0, NZ - 1)], recv_z
    ).wait()
    ig[...] = jnp.sum(z_recv[...], axis=0)

    to_partner.wait_send()
    pltpu.make_async_copy(psum.at[pl.ds(0, NZ - 1)], psum.at[pl.ds(0, NZ - 1)], send_z).wait()

    @pl.when(owner)
    def _():
        pltpu.make_async_copy(
            l_send.at[pl.ds(0, TILES - 1)], l_send.at[pl.ds(0, TILES - 1)], send_l
        ).wait()
        pltpu.make_async_copy(
            l_recv.at[pl.ds(0, NDP - 1)], l_recv.at[pl.ds(0, NDP - 1)], send_la
        ).wait()

    @pl.when(jnp.logical_not(owner))
    def _():
        pltpu.make_async_copy(l_send, l_send, send_l).wait()

    for sem in (send_s, send_sa, recv_sa):
        pltpu.make_async_copy(
            s_send.at[pl.ds(0, NDP - 1)], s_send.at[pl.ds(0, NDP - 1)], sem
        ).wait()


def finish_kernel(merged, b4, s_all, w, ig_in, new_w, new_e, ig, w_v, e_v, out_sem):
    copies = [pltpu.make_async_copy(ig_in, ig, out_sem.at[0])]
    copies[0].start()
    for n in range(NB):
        at = pl.ds(n * BLK, BLK)
        s_hi, s_lo = split(s_all[8 * n : 8 * n + 8].reshape(RANK, BLK))
        delta = dot(b4[...], jnp.concatenate([s_hi, s_lo, s_hi, s_lo], axis=0))
        e_v[:, at] = merged[:, at] - delta
        w_v[:, at] = w[:, at] - delta
        for i, (src, dst) in enumerate(((e_v, new_e), (w_v, new_w))):
            copies.append(
                pltpu.make_async_copy(src.at[:, at], dst.at[:, at], out_sem.at[1 + 2 * n + i])
            )
            copies[-1].start()
    for copy in copies:
        copy.wait()


def local(acts, out_grad, weight, error, start_q):
    hbm = pl.BlockSpec(memory_space=pltpu.HBM)
    vmem = pl.BlockSpec(memory_space=pltpu.VMEM)
    shape = jax.ShapeDtypeStruct
    dma = pltpu.SemaphoreType.DMA
    merged, b4, s_all, ig, weight_v = pl.pallas_call(
        comm_kernel,
        out_shape=(
            shape((DIN, COL), F32),
            shape((DIN, 4 * RANK), BF16),
            shape((NDP, 8, BLK), F32),
            shape((ROWS, DIN), F32),
            shape((DIN, COL), F32),
        ),
        in_specs=[hbm] * 5,
        out_specs=(vmem,) * 5,
        scratch_shapes=[
            pltpu.VMEM((TOK, DIN), BF16),
            pltpu.VMEM((TOK, COL), BF16),
            pltpu.VMEM((DIN, COL), F32),
            pltpu.VMEM((RANK, COL), F32),
            pltpu.VMEM((DIN, TOK), BF16),
            pltpu.VMEM((DIN, COL), BF16),
            pltpu.VMEM((DIN, COL), BF16),
            pltpu.VMEM((2 * RANK, COL), BF16),
            pltpu.VMEM((DIN, COL), BF16),
            pltpu.VMEM((DIN, COL), BF16),
            pltpu.VMEM((TILES, 8, 128), F32),
            pltpu.VMEM((NDP, 8, 128), F32),
            pltpu.VMEM((TILES, 8, 128), F32),
            pltpu.VMEM((NDP, 8, BLK), F32),
            pltpu.VMEM((NDP, 8, BLK), F32),
            pltpu.VMEM((2, NZ, ROWS, DIN), F32),
            pltpu.VMEM((NZ, ROWS, DIN), F32),
            pltpu.VMEM((NZ, ROWS, DIN), F32),
            pltpu.VMEM((NZ, ROWS, DIN), F32),
            dma((3 + 2 * NB,)),
        ]
        + [dma] * 12,
        compiler_params=pltpu.CompilerParams(
            collective_id=0, has_side_effects=True, vmem_limit_bytes=40 * 1024 * 1024
        ),
        name="powersgd_comm",
    )(*(pltpu.with_memory_space_constraint(a, pltpu.HBM) for a in (acts, out_grad, weight, error[0], start_q.T)))
    new_weight, new_error, input_grad = pl.pallas_call(
        finish_kernel,
        out_shape=(shape((DIN, COL), F32), shape((DIN, COL), F32), shape((ROWS, DIN), F32)),
        in_specs=[vmem] * 5,
        out_specs=(hbm,) * 3,
        scratch_shapes=[
            pltpu.VMEM((DIN, COL), F32),
            pltpu.VMEM((DIN, COL), F32),
            dma((1 + 2 * NB,)),
        ],
        compiler_params=pltpu.CompilerParams(vmem_limit_bytes=16 * 1024 * 1024),
        name="powersgd_finish",
    )(merged, b4, s_all, weight_v, ig)
    return new_weight, new_error[None], input_grad


def solution(mesh):
    placed = (
        P("dp", None),
        P("dp", "tensor"),
        P(None, "tensor"),
        P("dp", None, "tensor"),
        P("tensor", None),
    )
    return jax.shard_map(
        local,
        mesh=mesh,
        in_specs=placed,
        out_specs=(P(None, "tensor"), P("dp", None, "tensor"), P(("dp", "tensor"), None)),
        check_vma=False,
    )
```

```python
import functools

import jax
import jax.numpy as jnp
from jax import lax
from jax.experimental import pallas as pl
from jax.experimental.pallas import tpu as pltpu
from jax.sharding import PartitionSpec as P

HIGH = lax.Precision.HIGHEST
F32 = jnp.float32
BF16 = jnp.bfloat16
NN = (((1,), (0,)), ((), ()))
NT = (((1,), (1,)), ((), ()))

NX, NY = 4, 8
NDP = NX * NY
NZ = 8

DIN, COL, TOK, RANK = 256, 1024, 1024, 64
BLK = 256
LB = 2
WIDE = COL // LB
ROWS = TOK // (2 * NZ)
TILES = 16


def split(x):
    hi = x.astype(BF16)
    lo = (x - hi.astype(F32)).astype(BF16)
    return hi, lo


def dot(a, b, dims=NN):
    return lax.dot_general(a, b, dims, preferred_element_type=F32)


def sweeps(a, start, stop):
    n = a.shape[0]
    rows = lax.broadcasted_iota(jnp.int32, (n, n), 0)
    cols = lax.broadcasted_iota(jnp.int32, (n, n), 1)
    lane = lax.broadcasted_iota(jnp.int32, (1, n), 1)

    def sweep(k, a):
        at_row, at_col = rows == k, cols == k
        row = jnp.sum(jnp.where(at_row, a, 0.0), axis=0, keepdims=True)
        col = jnp.sum(jnp.where(at_col, a, 0.0), axis=1, keepdims=True)
        pivot = jnp.sum(jnp.where(lane == k, row, 0.0), axis=1, keepdims=True)
        inv = 1.0 / pivot
        scaled = row * inv
        out = a - col * scaled
        out = jnp.where(at_col, col * inv, out)
        return jnp.where(at_row, jnp.where(lane == k, -inv, scaled), out)

    return lax.fori_loop(start, stop, sweep, a)


FAR_X = (2, 1, 3, 0)
FAR_Y = (4, 3, 5, 2, 6, 1, 7, 0)
FAR_EVEN, FAR_ODD = (4, 2, 6, 0), (3, 5, 1, 7)
HALF = 36


def comm_kernel(
    acts_h, og_h, w_h, err_h, q_h,
    new_e, new_w, ig,
    merged, b4, s_all, w_v, acts_v, og_v, err_v, q_v,
    acts_t, mhi, mlo, qt, w_hi, w_lo,
    l_send, l_recv, l_all, s_send, s_recv, part, p_recv, psum, z_recv,
    load_sem, send_l, recv_l, send_la, recv_la, send_s, recv_s, send_sa, recv_sa,
    send_p, recv_p, send_z, recv_z,
):
    me = lax.axis_index("dp")
    x, y = me // NY, lax.rem(me, NY)
    t = lax.axis_index("tensor")
    z, core = t // 2, lax.rem(t, 2)

    loads = [
        pltpu.make_async_copy(q_h, q_v, load_sem.at[0]),
        pltpu.make_async_copy(acts_h, acts_v, load_sem.at[1]),
    ]
    for n in range(LB):
        at = pl.ds(n * WIDE, WIDE)
        loads.append(pltpu.make_async_copy(og_h.at[:, at], og_v.at[:, at], load_sem.at[2 + n]))
        loads.append(
            pltpu.make_async_copy(err_h.at[:, at], err_v.at[:, at], load_sem.at[2 + LB + n])
        )
    loads.append(pltpu.make_async_copy(w_h, w_v, load_sem.at[2 + 2 * LB]))
    for load in loads:
        load.start()

    xs = [lax.rem(x + d, NX) if d else x for d in FAR_X]
    ys = [lax.rem(y + d, NY) if d else y for d in FAR_Y]
    zs = [lax.rem(z + d, NZ) for d in FAR_Y[:-1]]
    peers = [px * NY + py for py in ys for px in xs][:-1]
    partner = z * 2 + 1 - core

    barrier = pltpu.get_barrier_semaphore()
    met = [{"dp": p} for p in peers] + [{"tensor": pz * 2 + core} for pz in zs]
    met.append({"tensor": partner})
    for device in met:
        pl.semaphore_signal(
            barrier, inc=1, device_id=device, device_id_type=pl.DeviceIdType.MESH
        )

    loads[0].wait()
    q_hi, q_lo = split(q_v[...])
    qt[0:RANK, :] = q_hi
    qt[RANK:, :] = q_lo
    loads[1].wait()
    acts_t[...] = acts_v[...].T
    both = jnp.zeros((2 * RANK, DIN), F32)
    left = jnp.zeros((RANK, DIN), F32)
    for n in range(LB):
        at = pl.ds(n * WIDE, WIDE)
        loads[2 + 2 * n].wait()
        loads[3 + 2 * n].wait()
        m = dot(acts_t[...], og_v[:, at]) * (TOK ** -0.5) + err_v[:, at]
        merged[:, at] = m
        hi, lo = split(m)
        mhi[:, at] = hi
        mlo[:, at] = lo
        both += dot(qt[:, at], hi, NT)
        left += dot(qt[0:RANK, at], lo, NT)
    left += both[0:RANK] + both[RANK:]
    l_send[0:8] = left[:, 0:128].reshape(8, 8, 128)
    l_send[8:16] = left[:, 128:256].reshape(8, 8, 128)

    pl.semaphore_wait(barrier, len(met))

    my_tile = x * 4 + y // 2
    owner = lax.rem(x + y, 2) == 0

    def left_copy(peer, tile):
        return pltpu.make_async_remote_copy(
            src_ref=l_send.at[tile], dst_ref=l_recv.at[me], send_sem=send_l, recv_sem=recv_l,
            device_id={"dp": peer}, device_id_type=pl.DeviceIdType.MESH,
        )

    odd = lax.rem(x + y, 2)
    same = [lax.rem(y + e + odd * (o - e), NY) for e, o in zip(FAR_EVEN, FAR_ODD)]
    other = [lax.rem(y + o + odd * (e - o), NY) for e, o in zip(FAR_EVEN, FAR_ODD)]
    for j in range(4):
        for dx, px in zip(FAR_X, xs):
            py = (other if dx % 2 else same)[j]
            copy = left_copy(px * NY + py, px * 4 + py // 2)
            if dx == 0 and j == 3:
                pl.when(jnp.logical_not(owner))(copy.start)
            else:
                copy.start()

    @pl.when(owner)
    def _():
        l_recv[me] = l_send[my_tile]

    loads[2 + 2 * LB].wait()
    wh, wl = split(w_v[...])
    w_hi[...] = wh
    w_lo[...] = wl

    def part_rows(i, _):
        rows = og_v[pl.ds(pl.multiple_of(i * 256, 256), 256), :]
        p = dot(rows, w_hi[...], NT) + dot(rows, w_lo[...], NT)
        p = p.reshape(2, 2, ROWS, DIN)
        for c in range(2):
            for half in range(2):
                part[c, 2 * i + half] = p[half, c]
        return _

    lax.fori_loop(0, TOK // 256, part_rows, 0)
    to_partner = pltpu.make_async_remote_copy(
        src_ref=part.at[1 - core], dst_ref=p_recv, send_sem=send_p, recv_sem=recv_p,
        device_id={"tensor": partner}, device_id_type=pl.DeviceIdType.MESH,
    )
    to_partner.start()

    def left_all(peer):
        return pltpu.make_async_remote_copy(
            src_ref=l_all.at[my_tile], dst_ref=l_all.at[my_tile], send_sem=send_la,
            recv_sem=recv_la, device_id={"dp": peer}, device_id_type=pl.DeviceIdType.MESH,
        )

    @pl.when(owner)
    def _():
        pltpu.make_async_copy(
            l_recv.at[pl.ds(0, NDP - 1)], l_recv.at[pl.ds(0, NDP - 1)], recv_l
        ).wait()
        l_all[my_tile] = jnp.sum(l_recv[...], axis=0) * (1.0 / NDP)

        for peer in peers:
            left_all(peer).start()

    to_partner.wait_recv()

    def pair_sum(i, _):
        psum[i] = part[core, i] + p_recv[i]
        return _

    lax.fori_loop(0, NZ, pair_sum, 0)

    def z_copy(pz):
        return pltpu.make_async_remote_copy(
            src_ref=psum.at[pz], dst_ref=z_recv.at[z], send_sem=send_z, recv_sem=recv_z,
            device_id={"tensor": pz * 2 + core}, device_id_type=pl.DeviceIdType.MESH,
        )

    for pz in zs:
        z_copy(pz).start()
    z_recv[z] = psum[z]

    @pl.when(owner)
    def _():
        pltpu.make_async_copy(
            l_all.at[pl.ds(0, TILES - 1)], l_all.at[pl.ds(0, TILES - 1)], recv_la
        ).wait()

    @pl.when(jnp.logical_not(owner))
    def _():
        pltpu.make_async_copy(l_all, l_all, recv_la).wait()

    left = jnp.concatenate(
        [l_all[0:8].reshape(RANK, 128), l_all[8:16].reshape(RANK, 128)], axis=1
    )
    l_hi, l_lo = split(left)
    l_both = jnp.concatenate([l_hi, l_lo], axis=0)
    for dx, px in zip(FAR_X, xs):
        at = pl.ds(pl.multiple_of(px * BLK, BLK), BLK)
        both = dot(l_both, mhi[:, at])
        s = both[0:RANK] + both[RANK:] + dot(l_hi, mlo[:, at])
        s_send[pl.ds(px * NY, NY)] = s.reshape(NY, 8, BLK)
        for dy, py in zip(FAR_Y, ys):
            if dx or dy:
                peer = px * NY + py
                pltpu.make_async_remote_copy(
                    src_ref=s_send.at[peer], dst_ref=s_recv.at[me], send_sem=send_s,
                    recv_sem=recv_s, device_id={"dp": peer},
                    device_id_type=pl.DeviceIdType.MESH,
                ).start()
    s_recv[me] = s_send[me]

    gram = lax.dot_general(left, left, NT, precision=HIGH, preferred_element_type=F32)
    swept = sweeps(gram, 0, HALF)

    pltpu.make_async_copy(
        s_recv.at[pl.ds(0, NDP - 1)], s_recv.at[pl.ds(0, NDP - 1)], recv_s
    ).wait()
    s_all[me] = jnp.sum(s_recv[...], axis=0)

    for peer in peers:
        pltpu.make_async_remote_copy(
            src_ref=s_all.at[me], dst_ref=s_all.at[me], send_sem=send_sa,
            recv_sem=recv_sa.at[x], device_id={"dp": peer}, device_id_type=pl.DeviceIdType.MESH,
        ).start()

    inv = -sweeps(swept, HALF, RANK)
    bt = lax.dot_general(inv, left, NN, precision=HIGH, preferred_element_type=F32)
    b_hi, b_lo = split(bt.T * (1.0 / NDP))
    b4[...] = jnp.concatenate([b_hi, b_hi, b_lo, b_lo], axis=1)

    pltpu.make_async_copy(
        z_recv.at[pl.ds(0, NZ - 1)], z_recv.at[pl.ds(0, NZ - 1)], recv_z
    ).wait()
    ig[...] = jnp.sum(z_recv[...], axis=0)

    for dx, px in reversed(tuple(zip(FAR_X, xs))):
        arrived = s_recv.at[pl.ds(0, NY if dx else NY - 1)]
        pltpu.make_async_copy(arrived, arrived, recv_sa.at[px]).wait()
        at = pl.ds(pl.multiple_of(px * BLK, BLK), BLK)
        s_hi, s_lo = split(s_all[pl.ds(px * NY, NY)].reshape(RANK, BLK))
        delta = dot(b4[...], jnp.concatenate([s_hi, s_lo, s_hi, s_lo], axis=0))
        new_e[:, at] = merged[:, at] - delta
        new_w[:, at] = w_v[:, at] - delta

    to_partner.wait_send()
    pltpu.make_async_copy(psum.at[pl.ds(0, NZ - 1)], psum.at[pl.ds(0, NZ - 1)], send_z).wait()

    @pl.when(owner)
    def _():
        pltpu.make_async_copy(
            l_send.at[pl.ds(0, TILES - 1)], l_send.at[pl.ds(0, TILES - 1)], send_l
        ).wait()
        pltpu.make_async_copy(
            l_recv.at[pl.ds(0, NDP - 1)], l_recv.at[pl.ds(0, NDP - 1)], send_la
        ).wait()

    @pl.when(jnp.logical_not(owner))
    def _():
        pltpu.make_async_copy(l_send, l_send, send_l).wait()

    for sem in (send_s, send_sa):
        pltpu.make_async_copy(
            s_send.at[pl.ds(0, NDP - 1)], s_send.at[pl.ds(0, NDP - 1)], sem
        ).wait()


def finish_kernel(e_v, w_v, ig_v, new_e, new_w, ig, out_sem):
    copies = []
    for src, dst in ((e_v, new_e), (w_v, new_w)):
        for half in range(2):
            at = pl.ds(half * (DIN // 2), DIN // 2)
            copies.append(
                pltpu.make_async_copy(src.at[at, :], dst.at[at, :], out_sem.at[len(copies)])
            )
    copies.append(pltpu.make_async_copy(ig_v, ig, out_sem.at[len(copies)]))
    for copy in copies:
        copy.start()
    for copy in copies:
        copy.wait()


def local(acts, out_grad, weight, error, start_q):
    hbm = pl.BlockSpec(memory_space=pltpu.HBM)
    vmem = pl.BlockSpec(memory_space=pltpu.VMEM)
    shape = jax.ShapeDtypeStruct
    dma = pltpu.SemaphoreType.DMA
    error_v, weight_v, ig = pl.pallas_call(
        comm_kernel,
        out_shape=(
            shape((DIN, COL), F32),
            shape((DIN, COL), F32),
            shape((ROWS, DIN), F32),
        ),
        in_specs=[hbm] * 5,
        out_specs=(vmem,) * 3,
        scratch_shapes=[
            pltpu.VMEM((DIN, COL), F32),
            pltpu.VMEM((DIN, 4 * RANK), BF16),
            pltpu.VMEM((NDP, 8, BLK), F32),
            pltpu.VMEM((DIN, COL), F32),
            pltpu.VMEM((TOK, DIN), BF16),
            pltpu.VMEM((TOK, COL), BF16),
            pltpu.VMEM((DIN, COL), F32),
            pltpu.VMEM((RANK, COL), F32),
            pltpu.VMEM((DIN, TOK), BF16),
            pltpu.VMEM((DIN, COL), BF16),
            pltpu.VMEM((DIN, COL), BF16),
            pltpu.VMEM((2 * RANK, COL), BF16),
            pltpu.VMEM((DIN, COL), BF16),
            pltpu.VMEM((DIN, COL), BF16),
            pltpu.VMEM((TILES, 8, 128), F32),
            pltpu.VMEM((NDP, 8, 128), F32),
            pltpu.VMEM((TILES, 8, 128), F32),
            pltpu.VMEM((NDP, 8, BLK), F32),
            pltpu.VMEM((NDP, 8, BLK), F32),
            pltpu.VMEM((2, NZ, ROWS, DIN), F32),
            pltpu.VMEM((NZ, ROWS, DIN), F32),
            pltpu.VMEM((NZ, ROWS, DIN), F32),
            pltpu.VMEM((NZ, ROWS, DIN), F32),
            dma((3 + 2 * LB,)),
        ]
        + [dma] * 7
        + [dma((NX,))]
        + [dma] * 4,
        compiler_params=pltpu.CompilerParams(
            collective_id=0, has_side_effects=True, vmem_limit_bytes=40 * 1024 * 1024
        ),
        name="powersgd_comm",
    )(*(pltpu.with_memory_space_constraint(a, pltpu.HBM) for a in (acts, out_grad, weight, error[0], start_q.T)))
    new_error, new_weight, input_grad = pl.pallas_call(
        finish_kernel,
        out_shape=(shape((DIN, COL), F32), shape((DIN, COL), F32), shape((ROWS, DIN), F32)),
        in_specs=[vmem] * 3,
        out_specs=(hbm,) * 3,
        scratch_shapes=[dma((5,))],
        compiler_params=pltpu.CompilerParams(vmem_limit_bytes=16 * 1024 * 1024),
        name="powersgd_finish",
    )(error_v, weight_v, ig)
    return new_weight, new_error[None], input_grad


def solution(mesh):
    placed = (
        P("dp", None),
        P("dp", "tensor"),
        P(None, "tensor"),
        P("dp", None, "tensor"),
        P("tensor", None),
    )
    return jax.shard_map(
        local,
        mesh=mesh,
        in_specs=placed,
        out_specs=(P(None, "tensor"), P("dp", None, "tensor"), P(("dp", "tensor"), None)),
        check_vma=False,
    )
```
